32 devices in a mesh: dp: 2 (over x), tp: 4 (over z), cp: 4 (over y, core).
Axes of the slice: x: 2, y: 2, z: 4, core: 2. Of those that a mesh axis runs over, the one named last changes fastest.
Arguments:
- x: bfloat16 [4096, 2048], P(('dp', 'cp')), parts along dimension 0
- doc_id: int32 [4096], P(('dp', 'cp')), parts along dimension 0
- pos_in_doc: int32 [4096], P(('dp', 'cp')), parts along dimension 0
- norm_gain: float32 [2048], replicated
- w_q: bfloat16 [2048, 2048], P(None, 'tp')
- w_k: bfloat16 [2048, 512], P(None, 'tp')
- w_v: bfloat16 [2048, 512], P(None, 'tp')
- w_o: bfloat16 [2048, 2048], P('tp')
- inv_freq: float32 [32], replicated
Outputs:
- output 1: bfloat16 [4096, 2048], P(('dp', 'cp')), parts along dimension 0
- output 2: bfloat16 [4096, 8, 64], P(('dp', 'cp'), 'tp'), parts along dimension 0
- output 3: bfloat16 [4096, 8, 64], P(('dp', 'cp'), 'tp'), parts along dimension 0
There are 2 independent parts. The reference program is written for one: setup_inputs(seed, part) draws one part's arguments, and reference() takes and returns one part's arrays. A program takes and returns all parts, laid end to end along the dimension named above; an argument that names none is the same for every part.
All inputs are finite; a program needn't handle non-finite values.
Results may differ from the reference program's by a relative error of at most 0.00417696.
Values are sent between devices in bfloat16 or wider.
A program may use at most 1 GiB of HBM per device.

```python
import jax
import jax.numpy as jnp
from jax import lax

TOKENS = 2048
CP_SIZE = 4
D_MODEL = 2048
Q_HEADS = 32
KV_HEADS = 8
HEAD_DIM = 64
DOC_LEN = 96
ROPE_THETA = 500000
QUERY_ROWS = 128

PIECE_LEN = TOKENS // (2 * CP_SIZE)
GROUP_SIZE = Q_HEADS // KV_HEADS
MAX_DOCS = TOKENS // (DOC_LEN // 2) + 2


def to_stored(glob_arr):
    pieces = glob_arr.reshape((2 * CP_SIZE, PIECE_LEN) + glob_arr.shape[1:])
    paired = jnp.stack([pieces[:CP_SIZE], pieces[CP_SIZE:][::-1]], axis=1)
    return paired.reshape(glob_arr.shape)


def draw_documents(doc_key):
    key_long, key_before, key_after = jax.random.split(doc_key, 3)
    first_piece = (DOC_LEN - 2) // PIECE_LEN + 1
    long_piece = jax.random.randint(key_long, (), first_piece, 2 * CP_SIZE)
    long_start = long_piece * PIECE_LEN - DOC_LEN + 1
    long_end = long_start + DOC_LEN
    lens_before = jax.random.randint(key_before, (MAX_DOCS,), DOC_LEN // 2, DOC_LEN + 1)
    lens_after = jax.random.randint(key_after, (MAX_DOCS,), DOC_LEN // 2, DOC_LEN + 1)
    starts_before = jnp.cumsum(lens_before)
    starts_after = long_end + jnp.cumsum(lens_after) - lens_after
    start_marks = jnp.zeros((TOKENS,), jnp.int32).at[0].set(1).at[long_start].set(1)
    start_marks = start_marks.at[jnp.where(starts_before < long_start, starts_before, TOKENS)].set(1, mode='drop')
    start_marks = start_marks.at[starts_after].set(1, mode='drop')
    doc_glob = jnp.cumsum(start_marks) - 1
    tok_index = jnp.arange(TOKENS)
    pos_glob = tok_index - lax.cummax(tok_index * start_marks, axis=0)
    return doc_glob.astype(jnp.int32), pos_glob.astype(jnp.int32)


def normal_weight(weight_key, fan_in, fan_out):
    return (jax.random.normal(weight_key, (fan_in, fan_out), jnp.float32) * fan_in ** -0.5).astype(jnp.bfloat16)


def setup_inputs(seed: int = 0, part: int = 0) -> dict:
    part_key = jax.random.fold_in(jax.random.key(seed), part)
    key_doc, key_noise, key_drift = jax.random.split(part_key, 3)
    shared = jax.random.split(jax.random.key(seed + 1), 6)
    doc_glob, pos_glob = draw_documents(key_doc)
    pos_ratio = pos_glob.astype(jnp.float32) / DOC_LEN
    drift_dir = jax.random.normal(key_drift, (D_MODEL,), jnp.float32)
    x_noise = jax.random.normal(key_noise, (TOKENS, D_MODEL), jnp.float32)
    x_glob = x_noise + 3.0 * pos_ratio[:, None] * drift_dir[None, :]
    norm_gain = 1.0 + 0.25 * jax.random.normal(shared[0], (D_MODEL,), jnp.float32)
    w_q = normal_weight(shared[1], D_MODEL, Q_HEADS * HEAD_DIM)
    w_k = normal_weight(shared[2], D_MODEL, KV_HEADS * HEAD_DIM)
    w_v = normal_weight(shared[3], D_MODEL, KV_HEADS * HEAD_DIM)
    w_o = normal_weight(shared[4], Q_HEADS * HEAD_DIM, D_MODEL)
    base_freq = ROPE_THETA ** (-jnp.arange(0, HEAD_DIM, 2, dtype=jnp.float32) / HEAD_DIM)
    inv_freq = base_freq * jnp.exp(0.1 * jax.random.normal(shared[5], (HEAD_DIM // 2,), jnp.float32))
    return {'x': to_stored(x_glob).astype(jnp.bfloat16), 'doc_id': to_stored(doc_glob), 'pos_in_doc': to_stored(pos_glob), 'norm_gain': norm_gain, 'w_q': w_q, 'w_k': w_k, 'w_v': w_v, 'w_o': w_o, 'inv_freq': inv_freq}


def apply_rope(vectors, cos_t, sin_t):
    half_dim = vectors.shape[-1] // 2
    lower_half = vectors[..., :half_dim].astype(jnp.float32)
    upper_half = vectors[..., half_dim:].astype(jnp.float32)
    turned = jnp.concatenate([lower_half * cos_t - upper_half * sin_t, upper_half * cos_t + lower_half * sin_t], axis=-1)
    return turned.astype(jnp.bfloat16)


def reference(x, doc_id, pos_in_doc, norm_gain, w_q, w_k, w_v, w_o, inv_freq):
    x_f32 = x.astype(jnp.float32)
    inv_rms = lax.rsqrt(jnp.mean(x_f32 * x_f32, axis=-1, keepdims=True) + 1e-5)
    normed = (x_f32 * inv_rms * norm_gain).astype(jnp.bfloat16)
    q_new = jnp.dot(normed, w_q, preferred_element_type=jnp.float32).astype(jnp.bfloat16).reshape(TOKENS, KV_HEADS, GROUP_SIZE, HEAD_DIM)
    k_new = jnp.dot(normed, w_k, preferred_element_type=jnp.float32).astype(jnp.bfloat16).reshape(TOKENS, KV_HEADS, HEAD_DIM)
    v_new = jnp.dot(normed, w_v, preferred_element_type=jnp.float32).astype(jnp.bfloat16).reshape(TOKENS, KV_HEADS, HEAD_DIM)
    rope_angle = pos_in_doc.astype(jnp.float32)[:, None] * inv_freq[None, :]
    cos_t = jnp.cos(rope_angle)
    sin_t = jnp.sin(rope_angle)
    q_rot = apply_rope(q_new, cos_t[:, None, None, :], sin_t[:, None, None, :])
    k_rot = apply_rope(k_new, cos_t[:, None, :], sin_t[:, None, :])
    tok_index = to_stored(jnp.arange(TOKENS))
    k_f32 = k_rot.astype(jnp.float32)
    v_f32 = v_new.astype(jnp.float32)
    blocks = TOKENS // QUERY_ROWS

    def attend(block_args):
        q_blk, doc_blk, idx_blk = block_args
        scores = jnp.einsum('qngd,knd->ngqk', q_blk.astype(jnp.float32), k_f32) * (HEAD_DIM ** -0.5)
        visible = (doc_blk[:, None] == doc_id[None, :]) & (tok_index[None, :] <= idx_blk[:, None])
        scores = jnp.where(visible, scores, -1e30)
        attn_probs = jax.nn.softmax(scores, axis=-1).astype(jnp.bfloat16).astype(jnp.float32)
        return jnp.einsum('ngqk,knd->qngd', attn_probs, v_f32).astype(jnp.bfloat16)

    attn_out = lax.map(attend, (q_rot.reshape(blocks, QUERY_ROWS, KV_HEADS, GROUP_SIZE, HEAD_DIM), doc_id.reshape(blocks, QUERY_ROWS), tok_index.reshape(blocks, QUERY_ROWS)))
    mixed_out = jnp.dot(attn_out.reshape(TOKENS, Q_HEADS * HEAD_DIM), w_o, preferred_element_type=jnp.float32)
    y_out = (x_f32 + mixed_out).astype(jnp.bfloat16)
    return (y_out, k_rot, v_new)
```

```python
import functools

import jax
import jax.numpy as jnp
from jax import lax
from jax.experimental import pallas as pl
from jax.experimental.pallas import tpu as pltpu
from jax.sharding import PartitionSpec as P

MESH = pl.DeviceIdType.MESH
F32 = jnp.float32
BF16 = jnp.bfloat16
ROWS = 512
BLK = 128
PIECE = 256
DM = 2048
TP = 4
SUB = 4
NEG = -1e30


def rcopy(src, dst, ssem, rsem, dev):
    return pltpu.make_async_remote_copy(src_ref=src, dst_ref=dst, send_sem=ssem, recv_sem=rsem, device_id=dev, device_id_type=MESH)


def places():
    dp, tp, cp = lax.axis_index('dp'), lax.axis_index('tp'), lax.axis_index('cp')
    y, c = cp // 2, cp % 2
    return dp, tp, cp, y, c


def rotate(t, cos_t, sin_t, low):
    turned = jnp.where(low, pltpu.roll(t, 96, 1), pltpu.roll(t, 32, 1))
    return t * cos_t + turned * sin_t


def front_kernel(x_ref, pos_ref, gain_ref, freq_ref, wq_ref, wk_ref, wv_ref, wo_ref,
                 q_ref, k_ref, v_ref, kv_out, wol_ref,
                 xv, wqv, wkv, h, cosv, sinv, kv_all, lsem, osem,
                 kv_ss, kv_rs, wz_ss, wz_rs):
    dp, tp, cp, y, c = places()
    lane_row = (dp * 4 + cp) * 64
    partner = (dp, tp, 2 * y + 1 - c)
    ynb = (dp, tp, 2 * (1 - y) + c)
    right, left = (dp, tp + 1, cp), (dp, tp - 1, cp)

    loads = []
    for b in range(4):
        loads.append(pltpu.make_async_copy(x_ref.at[pl.ds(b * BLK, BLK)], xv.at[pl.ds(b * BLK, BLK)], lsem.at[b]))
    loads.append(pltpu.make_async_copy(wk_ref, wkv.at[:, pl.ds(0, 128)], lsem.at[4]))
    loads.append(pltpu.make_async_copy(wv_ref, wkv.at[:, pl.ds(128, 128)], lsem.at[5]))
    loads.append(pltpu.make_async_copy(wq_ref, wqv, lsem.at[6]))
    for cpy in loads:
        cpy.start()

    barrier = pltpu.get_barrier_semaphore()
    for dev in (partner, ynb):
        pl.semaphore_signal(barrier, inc=1, device_id=dev, device_id_type=MESH)

    @pl.when(tp < TP - 1)
    def _():
        pl.semaphore_signal(barrier, inc=1, device_id=right, device_id_type=MESH)

    @pl.when(tp > 0)
    def _():
        pl.semaphore_signal(barrier, inc=1, device_id=left, device_id_type=MESH)

    lane = lax.broadcasted_iota(jnp.int32, (BLK, 128), 1)
    low = (lane % 64) < 32
    pos_t = pos_ref[...].T
    for b in range(4):
        ang = pos_t[:, b:b + 1] * freq_ref[...]
        rows = pl.ds(b * BLK, BLK)
        cosv[rows, :] = jnp.cos(ang)
        s = jnp.sin(ang)
        sinv[rows, :] = jnp.where(low, -s, s)

    pl.semaphore_wait(barrier, 3 + tp * (3 - tp) // 2)

    def wz(direction, src, half, own):
        part = pl.ds(half * 32, 32)
        src_ref = wo_ref.at[pl.ds(lane_row + half * 32, 32)] if own else wol_ref.at[src, part]
        return rcopy(src_ref, wol_ref.at[src, part], wz_ss.at[direction, src, half], wz_rs.at[src, half], right if direction == 0 else left)

    @pl.when(tp < TP - 1)
    def _():
        for half in range(2):
            wz(0, tp, half, True).start()

    @pl.when(tp > 0)
    def _():
        for half in range(2):
            wz(1, tp, half, True).start()

    def wz_step(s, half):
        @pl.when(tp >= s)
        def _():
            wz(0, tp - s, half, False).wait_recv()

        @pl.when((tp >= s) & (tp < TP - 1))
        def _():
            wz(0, tp - s, half, False).start()

        @pl.when(tp + s < TP)
        def _():
            wz(1, tp + s, half, False).wait_recv()

        @pl.when((tp + s < TP) & (tp > 0))
        def _():
            wz(1, tp + s, half, False).start()

    for b in range(4):
        rows = pl.ds(b * BLK, BLK)
        loads[b].wait()
        xf = xv[rows, :].astype(F32)
        inv = lax.rsqrt(jnp.mean(xf * xf, axis=-1, keepdims=True) + 1e-5)
        h[rows, :] = (xf * inv * gain_ref[...]).astype(BF16)

    loads[4].wait()
    loads[5].wait()
    my_a, my_b = cp * PIECE, (7 - cp) * PIECE
    nb_cp = 2 * (1 - y) + c
    nb = (nb_cp * PIECE, (7 - nb_cp) * PIECE)
    pt_cp = 2 * y + 1 - c
    pt = (pt_cp * PIECE, (7 - pt_cp) * PIECE)
    pd_cp = 2 * (1 - y) + 1 - c
    pd = (pd_cp * PIECE, (7 - pd_cp) * PIECE)
    mine = (my_a, my_b)

    def kvc(kind, half, row, dev):
        piece = kv_all.at[pl.ds(row, PIECE)]
        return rcopy(piece, piece, kv_ss.at[kind, half], kv_rs.at[kind, half], dev)

    for half in range(2):
        for bb in range(2):
            b = half * 2 + bb
            rows = pl.ds(b * BLK, BLK)
            kv = jnp.dot(h[rows, :], wkv[...], preferred_element_type=F32).astype(BF16)
            kf = kv[:, 0:128].astype(F32)
            k_rot = rotate(kf, cosv[rows, :], sinv[rows, :], low).astype(BF16)
            k_ref[:, rows] = k_rot.astype(F32).T.astype(BF16)
            v_ref[:, rows] = kv[:, 128:256].astype(F32).T.astype(BF16)
            dst = pl.ds(mine[half] + bb * BLK, BLK)
            kv_all[dst, 0:128] = k_rot
            kv_all[dst, 128:256] = kv[:, 128:256]
        kvc(0, half, mine[half], ynb).start()
        kvc(1, half, mine[half], partner).start()

    loads[6].wait()

    def q_rows(b):
        rows = pl.ds(b * BLK, BLK)
        qf = jnp.dot(h[rows, :], wqv[...], preferred_element_type=F32).astype(BF16).astype(F32)
        for g in range(4):
            cols = pl.ds(g * 128, 128)
            q_ref[rows, cols] = rotate(qf[:, g * 128:(g + 1) * 128], cosv[rows, :], sinv[rows, :], low).astype(BF16)

    q_rows(0)
    q_rows(1)
    wz_step(1, 0)
    q_rows(2)
    q_rows(3)
    wz_step(1, 1)
    wz_step(2, 0)
    for half in range(2):
        kvc(0, half, nb[half], ynb).wait_recv()
        kvc(2, half, nb[half], partner).start()
    wz_step(2, 1)
    for half in range(2):
        kvc(1, half, pt[half], partner).wait_recv()
        kvc(2, half, pd[half], partner).wait_recv()
    out = pltpu.make_async_copy(kv_all, kv_out, osem.at[0])
    out.start()
    wz_step(3, 0)
    wz_step(3, 1)
    for half in range(2):
        kvc(0, half, mine[half], ynb).wait_send()
        kvc(1, half, mine[half], partner).wait_send()
        kvc(2, half, nb[half], partner).wait_send()
    for s in range(0, TP):
        for half in range(2):
            @pl.when((tp >= s) & (tp < TP - 1))
            def _():
                wz(0, tp - s, half, s == 0).wait_send()

            @pl.when((tp + s < TP) & (tp > 0))
            def _():
                wz(1, tp + s, half, s == 0).wait_send()
    out.wait()


def front(x, pos8, gain, freq, wq, wk, wv, wo):
    any_, vm = pl.BlockSpec(memory_space=pl.ANY), pl.BlockSpec(memory_space=pltpu.VMEM)
    sds = jax.ShapeDtypeStruct
    dma = pltpu.SemaphoreType.DMA
    return pl.pallas_call(
        front_kernel,
        out_shape=(sds((ROWS, 512), BF16), sds((128, ROWS), BF16), sds((128, ROWS), BF16), sds((2048, 256), BF16), sds((TP, 64, DM), BF16)),
        in_specs=[any_, vm, vm, vm, any_, any_, any_, any_],
        out_specs=(vm, vm, vm, any_, any_),
        scratch_shapes=[
            pltpu.VMEM((ROWS, DM), BF16), pltpu.VMEM((DM, 512), BF16), pltpu.VMEM((DM, 256), BF16), pltpu.VMEM((ROWS, DM), BF16),
            pltpu.VMEM((ROWS, 128), F32), pltpu.VMEM((ROWS, 128), F32), pltpu.VMEM((2048, 256), BF16),
            dma((7,)), dma((1,)), dma((3, 2)), dma((3, 2)), dma((2, TP, 2)), dma((TP, 2)),
        ],
        compiler_params=pltpu.CompilerParams(collective_id=0, has_side_effects=True, vmem_limit_bytes=60 * 1024 * 1024),
        name='front',
    )(x, pos8, gain, freq, wq, wk, wv, wo)


def attend_kernel(first_ref, q_ref, kv_ref, pos_ref, o_ref, s_e, s_o):
    cp = lax.axis_index('cp')
    pos_t = pos_ref[...].T.astype(jnp.int32)
    low = lax.broadcasted_iota(jnp.int32, (1, 128), 1) < 64

    def halves(mat, n):
        zero = jnp.zeros_like(mat)
        other = pltpu.roll(mat.astype(F32), 64, 1).astype(BF16)
        if n == 0:
            return jnp.where(low, mat, zero), jnp.where(low, zero, other)
        return jnp.where(low, other, zero), jnp.where(low, zero, mat)

    def dot_t(a, b):
        return lax.dot_general(a, b, (((1,), (1,)), ((), ())), preferred_element_type=F32)

    def bias_of(base, width, t, p):
        u = base + lax.broadcasted_iota(jnp.int32, (BLK, width), 1)
        one = jnp.where((u <= t) & (u >= t - p), 0.0, NEG)
        return jnp.concatenate([one, one], axis=0)

    for b in range(4):
        piece = cp if b < 2 else 7 - cp
        t0 = piece * PIECE + (b % 2) * BLK
        p = pos_t[:, b:b + 1]
        t = t0 + lax.broadcasted_iota(jnp.int32, (BLK, 1), 0)
        first = t0 - first_ref[b]
        diag = t0 // BLK
        lo = first // BLK
        rows = pl.ds(b * BLK, BLK)

        def q_pairs(n):
            return jnp.concatenate([q_ref[rows, pl.ds(n * 256, 128)], q_ref[rows, pl.ds(n * 256 + 128, 128)]], axis=0)

        def put(n, out):
            o_ref[rows, pl.ds(n * 256, 128)] = out[0:BLK].astype(BF16)
            o_ref[rows, pl.ds(n * 256 + 128, 128)] = out[BLK:].astype(BF16)

        @pl.when(lo >= diag - 1)
        def _():
            base = jnp.maximum(diag - 1, 0) * BLK
            keys = pl.ds(pl.multiple_of(base, BLK), 2 * BLK)
            bias = bias_of(base, 2 * BLK, t, p)
            kk, vv = kv_ref[keys, 0:128], kv_ref[keys, 128:256]
            for n in range(2):
                qq = q_pairs(n)
                out = jnp.zeros((2 * BLK, 128), F32)
                for km, vm in zip(halves(kk, n), halves(vv, n)):
                    s = dot_t(qq, km) * 0.125 + bias
                    e = jnp.exp(s - jnp.max(s, axis=-1, keepdims=True))
                    pr = (e * (1.0 / jnp.sum(e, axis=-1, keepdims=True))).astype(BF16)
                    out = out + jnp.dot(pr, vm, preferred_element_type=F32)
                put(n, out)

        @pl.when(lo < diag - 1)
        def _():
            for n in range(2):
                qq = q_pairs(n)

                def score(kb, ms):
                    keys = pl.ds(pl.multiple_of(kb * BLK, BLK), BLK)
                    bias = bias_of(kb * BLK, BLK, t, p)
                    new = []
                    for km, s_ref, m in zip(halves(kv_ref[keys, 0:128], n), (s_e, s_o), ms):
                        s = dot_t(qq, km) * 0.125 + bias
                        s_ref[kb] = s
                        new.append(jnp.maximum(m, jnp.max(s, axis=-1, keepdims=True)))
                    return tuple(new)

                m0 = jnp.full((2 * BLK, 1), NEG, F32)
                ms = lax.fori_loop(lo, diag + 1, score, (m0, m0))

                def total(kb, ls):
                    return tuple(l + jnp.sum(jnp.exp(s_ref[kb] - m), axis=-1, keepdims=True) for l, s_ref, m in zip(ls, (s_e, s_o), ms))

                z0 = jnp.zeros((2 * BLK, 1), F32)
                ls = lax.fori_loop(lo, diag + 1, total, (z0, z0))
                rs = tuple(1.0 / l for l in ls)

                def mix(kb, out):
                    keys = pl.ds(pl.multiple_of(kb * BLK, BLK), BLK)
                    for vm, s_ref, m, r in zip(halves(kv_ref[keys, 128:256], n), (s_e, s_o), ms, rs):
                        pr = (jnp.exp(s_ref[kb] - m) * r).astype(BF16)
                        out = out + jnp.dot(pr, vm, preferred_element_type=F32)
                    return out

                put(n, lax.fori_loop(lo, diag + 1, mix, jnp.zeros((2 * BLK, 128), F32)))


def attend(first, q, kv, pos8):
    vm = pl.BlockSpec(memory_space=pltpu.VMEM)
    return pl.pallas_call(
        attend_kernel,
        out_shape=jax.ShapeDtypeStruct((ROWS, 512), BF16),
        in_specs=[pl.BlockSpec(memory_space=pltpu.SMEM), vm, vm, vm],
        out_specs=vm,
        scratch_shapes=[pltpu.VMEM((16, 2 * BLK, BLK), F32), pltpu.VMEM((16, 2 * BLK, BLK), F32)],
        compiler_params=pltpu.CompilerParams(vmem_limit_bytes=24 * 1024 * 1024),
        name='attend',
    )(first, q, kv, pos8)


def out_kernel(o_ref, x_ref, wo_ref, wol_ref, y_ref, o_all, wo_all, acc, xv, lsem, o_ss, o_rs, w_ss, f_ss, w_rs):
    dp, tp, cp, y, c = places()
    lane = dp * 4 + cp
    partner = (dp, tp, 2 * y + 1 - c)
    xnb = (1 - dp, tp, cp)
    ynb = (dp, tp, 2 * (1 - y) + c)
    dnb = (1 - dp, tp, 2 * (1 - y) + c)
    right, left = (dp, tp + 1, cp), (dp, tp - 1, cp)
    lanes = ((1 - dp) * 4 + cp, dp * 4 + 2 * (1 - y) + c, (1 - dp) * 4 + 2 * (1 - y) + c)
    peers = (xnb, ynb, dnb)
    p_lanes = tuple(l + 1 - 2 * c for l in (lane,) + lanes)

    mid, flip = tp * (3 - tp) // 2, tp // 2
    order = []
    for base in (1 + mid, 2 - 2 * mid, 3):
        order.append(base + flip * (3 - 2 * base))

    load_o = pltpu.make_async_copy(o_ref, o_all.at[tp], lsem.at[0])
    load_o.start()

    def slot(j, l):
        return wo_all.at[j, pl.ds(l * 64, 64)]

    load_l = [pltpu.make_async_copy(wol_ref.at[j], slot(j, lane), lsem.at[3 + i]) for i, j in enumerate(order)]
    for cpy in load_l:
        cpy.start()
    load_w = pltpu.make_async_copy(wo_ref, wo_all.at[tp], lsem.at[1])
    load_w.start()
    load_x = pltpu.make_async_copy(x_ref, xv, lsem.at[2])
    load_x.start()

    barrier = pltpu.get_barrier_semaphore()
    for dev in (partner,) + peers:
        pl.semaphore_signal(barrier, inc=1, device_id=dev, device_id_type=MESH)

    @pl.when(tp < TP - 1)
    def _():
        pl.semaphore_signal(barrier, inc=1, device_id=right, device_id_type=MESH)

    @pl.when(tp > 0)
    def _():
        pl.semaphore_signal(barrier, inc=1, device_id=left, device_id_type=MESH)

    pl.semaphore_wait(barrier, 5 + mid)

    def oc(direction, src, sub):
        part = o_all.at[src, pl.ds(sub * BLK, BLK)]
        return rcopy(part, part, o_ss.at[direction, src, sub], o_rs.at[src, sub], right if direction == 0 else left)

    load_o.wait()

    @pl.when(tp < TP - 1)
    def _():
        for sub in range(SUB):
            oc(0, tp, sub).start()

    @pl.when(tp > 0)
    def _():
        for sub in range(SUB):
            oc(1, tp, sub).start()

    def wsend(k, i, j, l, dev):
        return rcopy(slot(j, l), slot(j, l), w_ss.at[k, i], w_rs.at[j, l], dev)

    def wforward(k, i, j, l):
        return rcopy(slot(j, l), slot(j, l), f_ss.at[k, i], w_rs.at[j, l], partner)

    for k, j in enumerate(order):
        load_l[k].wait()
        for i, dev in enumerate(peers + (partner,)):
            wsend(k, i, j, lane, dev).start()

    def product(j, last):
        for n in range(4):
            cols = pl.ds(n * 512, 512)
            part = jnp.dot(o_all[j], wo_all[j, :, n * 512:(n + 1) * 512], preferred_element_type=F32)
            if last:
                y_ref[:, cols] = (acc[:, cols] + part).astype(BF16)
            else:
                acc[:, cols] += part

    load_w.wait()
    load_x.wait()
    for n in range(4):
        cols = pl.ds(n * 512, 512)
        acc[:, cols] = xv[:, cols].astype(F32)
    product(tp, False)

    def o_step(s, sub):
        @pl.when(tp >= s)
        def _():
            oc(0, tp - s, sub).wait_recv()

        @pl.when((tp >= s) & (tp < TP - 1))
        def _():
            oc(0, tp - s, sub).start()

        @pl.when(tp + s < TP)
        def _():
            oc(1, tp + s, sub).wait_recv()

        @pl.when((tp + s < TP) & (tp > 0))
        def _():
            oc(1, tp + s, sub).start()

    def w_step(k, i):
        j = order[k]
        wsend(k, i, j, lanes[i], peers[i]).wait_recv()
        wforward(k, i, j, lanes[i]).start()

    for k in range(3):
        s = k + 1
        o_step(s, 0)
        o_step(s, 1)
        w_step(k, 0)
        w_step(k, 1)
        o_step(s, 2)
        o_step(s, 3)
        w_step(k, 2)
        for l in p_lanes:
            wforward(k, 0, order[k], l).wait_recv()
        product(order[k], k == 2)

    for k, j in enumerate(order):
        for i, dev in enumerate(peers + (partner,)):
            wsend(k, i, j, lane, dev).wait_send()
        for i in range(3):
            wforward(k, i, j, lanes[i]).wait_send()
    for s in range(0, TP):
        for sub in range(SUB):
            @pl.when((tp >= s) & (tp < TP - 1))
            def _():
                oc(0, tp - s, sub).wait_send()

            @pl.when((tp + s < TP) & (tp > 0))
            def _():
                oc(1, tp + s, sub).wait_send()


def project_out(o, x, wo, wol):
    any_, vm = pl.BlockSpec(memory_space=pl.ANY), pl.BlockSpec(memory_space=pltpu.VMEM)
    dma = pltpu.SemaphoreType.DMA
    return pl.pallas_call(
        out_kernel,
        out_shape=jax.ShapeDtypeStruct((ROWS, DM), BF16),
        in_specs=[any_, any_, any_, any_],
        out_specs=vm,
        scratch_shapes=[
            pltpu.VMEM((TP, ROWS, 512), BF16), pltpu.VMEM((TP, 512, DM), BF16), pltpu.VMEM((ROWS, DM), F32), pltpu.VMEM((ROWS, DM), BF16),
            dma((6,)), dma((2, TP, SUB)), dma((TP, SUB)), dma((3, 4)), dma((3, 3)), dma((TP, 8)),
        ],
        compiler_params=pltpu.CompilerParams(collective_id=1, has_side_effects=True, vmem_limit_bytes=60 * 1024 * 1024),
        name='project_out',
    )(o, x, wo, wol)


def solution(mesh):
    def local_step(x, doc_id, pos, gain, wq, wk, wv, wo, inv_freq):
        pos8 = jnp.pad(pos.reshape(4, BLK).astype(F32), ((0, 4), (0, 0)))
        freq = jnp.tile(inv_freq.reshape(1, 32), (1, 4))
        first = pos.reshape(4, BLK)[:, 0]
        q, k, v, kv, wol = front(x, pos8, gain.reshape(1, DM), freq, wq, wk, wv, wo)
        o = attend(first, q, kv, pos8)
        y = project_out(o, x, wo, wol)
        return y, k.T.reshape(ROWS, 2, 64), v.T.reshape(ROWS, 2, 64)

    row_spec = P(('dp', 'cp'))
    in_specs = (P(('dp', 'cp'), None), row_spec, row_spec, P(), P(None, 'tp'), P(None, 'tp'), P(None, 'tp'), P('tp', None), P())
    out_specs = (P(('dp', 'cp'), None), P(('dp', 'cp'), 'tp', None), P(('dp', 'cp'), 'tp', None))
    return jax.shard_map(local_step, mesh=mesh, in_specs=in_specs, out_specs=out_specs, check_vma=False)
```

```python
import jax
import jax.numpy as jnp
from jax import lax
from jax.experimental import pallas as pl
from jax.experimental.pallas import tpu as pltpu
from jax.sharding import PartitionSpec as P

MESH = pl.DeviceIdType.MESH
F32 = jnp.float32
BF16 = jnp.bfloat16
ROWS = 512
BLK = 128
PIECE = 256
DM = 2048
TP = 4
NEG = -1e30


def rcopy(src, dst, ssem, rsem, dev):
    return pltpu.make_async_remote_copy(src_ref=src, dst_ref=dst, send_sem=ssem, recv_sem=rsem, device_id=dev, device_id_type=MESH)


def layer_kernel(x_ref, pos_ref, gain_ref, freq_ref, wq_ref, wk_ref, wv_ref, wo_ref,
                 y_ref, kt_ref, vt_ref,
                 xv, wqv, wkv, h, cosv, sinv, kv_all, kk, vv, qm, st, m_s, l_s, a_s, o_all, wo_all, acc,
                 lsem, kv_ss, kv_rs, wz_ss, w_ss, f_ss, w_rs, o_ss, o_rs):
    dp, tp, cp = lax.axis_index('dp'), lax.axis_index('tp'), lax.axis_index('cp')
    y, c = cp // 2, cp % 2
    lane = dp * 4 + cp
    partner = (dp, tp, 2 * y + 1 - c)
    xnb = (1 - dp, tp, cp)
    ynb = (dp, tp, 2 * (1 - y) + c)
    dnb = (1 - dp, tp, 2 * (1 - y) + c)
    right, left = (dp, tp + 1, cp), (dp, tp - 1, cp)
    lanes = ((1 - dp) * 4 + cp, dp * 4 + 2 * (1 - y) + c, (1 - dp) * 4 + 2 * (1 - y) + c)
    peers = (xnb, ynb, dnb)
    p_lanes = tuple(l + 1 - 2 * c for l in (lane,) + lanes)
    mid, flip = tp * (3 - tp) // 2, tp // 2
    order = []
    for base in (1 + mid, 2 - 2 * mid, 3):
        order.append(base + flip * (3 - 2 * base))

    barrier = pltpu.get_barrier_semaphore()
    for dev in (partner,) + peers + tuple((dp, j, cp) for j in order):
        pl.semaphore_signal(barrier, inc=1, device_id=dev, device_id_type=MESH)

    loads = []
    for b in range(2):
        rows = pl.ds(b * PIECE, PIECE)
        loads.append(pltpu.make_async_copy(x_ref.at[rows], xv.at[rows], lsem.at[b]))
    loads.append(pltpu.make_async_copy(wk_ref, wkv.at[:, pl.ds(0, 128)], lsem.at[2]))
    loads.append(pltpu.make_async_copy(wv_ref, wkv.at[:, pl.ds(128, 128)], lsem.at[3]))
    loads.append(pltpu.make_async_copy(wq_ref, wqv, lsem.at[4]))
    loads.append(pltpu.make_async_copy(wo_ref, wo_all.at[tp], lsem.at[5]))
    for cpy in loads:
        cpy.start()

    lane_i = lax.broadcasted_iota(jnp.int32, (BLK, 128), 1)
    pos_t = jnp.concatenate([pos_ref[...].astype(F32), jnp.zeros((4, BLK), F32)], axis=0).T
    freq = jnp.concatenate([freq_ref[...]] * 4, axis=1)
    pos_l = jnp.zeros((BLK, 128), F32)
    for b in range(4):
        pos_l = jnp.where(lane_i // 32 == b, pos_t[:, b:b + 1], pos_l)
    ang = pos_l * freq
    tables = (jnp.cos(ang), jnp.sin(ang))
    low32 = (lane_i % 64) < 32
    for b in range(4):
        for ref, tab in zip((cosv, sinv), tables):
            t = jnp.where(lane_i // 32 == b, tab, 0.0)
            t = t + pltpu.roll(t, 32, 1)
            t = t + pltpu.roll(t, 64, 1)
            if ref is sinv:
                t = jnp.where(low32, -t, t)
            ref[b * BLK:(b + 1) * BLK, :] = t

    pl.semaphore_wait(barrier, 7)

    def slot(j, l):
        return wo_all.at[j, pl.ds(l * 64, 64)]

    for k, j in enumerate(order):
        rcopy(wo_ref.at[pl.ds(lane * 64, 64)], slot(tp, lane), wz_ss.at[k], w_rs.at[tp, lane], (dp, j, cp)).start()

    def wz(k):
        return rcopy(slot(order[k], lane), slot(order[k], lane), wz_ss.at[k], w_rs.at[order[k], lane], (dp, order[k], cp))

    def wsend(k, i, l, dev):
        return rcopy(slot(order[k], l), slot(order[k], l), w_ss.at[k, i], w_rs.at[order[k], l], dev)

    def wforward(k, i, l):
        return rcopy(slot(order[k], l), slot(order[k], l), f_ss.at[k, i], w_rs.at[order[k], l], partner)

    def w_arrive(k):
        wz(k).wait_recv()
        for i, dev in enumerate(peers + (partner,)):
            wsend(k, i, lane, dev).start()

    def w_step(k, i):
        wsend(k, i, lanes[i], peers[i]).wait_recv()
        wforward(k, i, lanes[i]).start()

    def norm(b):
        rows = pl.ds(b * PIECE, PIECE)
        xf = xv[rows, :].astype(F32)
        inv = lax.rsqrt(jnp.mean(xf * xf, axis=-1, keepdims=True) + 1e-5)
        h[rows, :] = (xf * inv * gain_ref[...]).astype(BF16)

    low = lax.broadcasted_iota(jnp.int32, (PIECE, 128), 1)
    low_head = low < 64
    low_half = (low % 64) < 32

    def rotate(t, rows):
        turned = jnp.where(low_half, pltpu.roll(t, 96, 1), pltpu.roll(t, 32, 1))
        return t * cosv[rows, :] + turned * sinv[rows, :]

    mine = (cp, 7 - cp)
    nb_cp, pt_cp, pd_cp = 2 * (1 - y) + c, 2 * y + 1 - c, 2 * (1 - y) + 1 - c
    nb, pt, pd = (nb_cp, 7 - nb_cp), (pt_cp, 7 - pt_cp), (pd_cp, 7 - pd_cp)

    def kvc(kind, half, piece, dev):
        return rcopy(kv_all.at[piece], kv_all.at[piece], kv_ss.at[kind, half], kv_rs.at[kind, half], dev)

    for b in range(2):
        rows = slice(b * PIECE, (b + 1) * PIECE)
        loads[b].wait()
        norm(b)
        if b == 0:
            loads[2].wait()
            loads[3].wait()
        kv = jnp.dot(h[rows, :], wkv[...], preferred_element_type=F32).astype(BF16)
        k_rot = rotate(kv[:, 0:128].astype(F32), rows).astype(BF16)
        kv_all[mine[b], :, 0:128] = k_rot
        kv_all[mine[b], :, 128:256] = kv[:, 128:256]
        kt_ref[:, rows] = k_rot.astype(F32).T.astype(BF16)
        vt_ref[:, rows] = kv[:, 128:256].astype(F32).T.astype(BF16)
        kvc(0, b, mine[b], ynb).start()
        kvc(1, b, mine[b], partner).start()

    loads[4].wait()
    for b in range(2):
        rows = slice(b * PIECE, (b + 1) * PIECE)
        qf = jnp.dot(h[rows, :], wqv[...], preferred_element_type=F32).astype(BF16).astype(F32)
        for g in range(4):
            q = rotate(qf[:, g * 128:(g + 1) * 128], rows).astype(BF16)
            q = (q.astype(F32) * 0.125).astype(BF16)
            zero = jnp.zeros_like(q)
            at = (g % 2) * 2 * PIECE
            qm[g // 2, b, at:at + PIECE, :] = jnp.where(low_head, q, zero)
            qm[g // 2, b, at + PIECE:at + 2 * PIECE, :] = jnp.where(low_head, zero, q)

    w_arrive(0)
    for b in range(2):
        kvc(0, b, nb[b], ynb).wait_recv()
        kvc(2, b, nb[b], partner).start()
    for b in range(2):
        kvc(1, b, pt[b], partner).wait_recv()
        kvc(2, b, pd[b], partner).wait_recv()

    def double(piece, carry):
        for i, ref in enumerate((kk, vv)):
            t = kv_all[piece, :, i * 128:(i + 1) * 128]
            r = pltpu.roll(t.astype(F32), 64, 1).astype(BF16)
            ref[0, piece] = jnp.where(low_head, t, r)
            ref[1, piece] = jnp.where(low_head, r, t)
        return carry

    lax.fori_loop(0, 8, double, 0)

    q_iota = lax.broadcasted_iota(jnp.int32, (PIECE, PIECE), 0)
    k_iota = lax.broadcasted_iota(jnp.int32, (PIECE, PIECE), 1)

    def attend(n, b):
        piece = mine[b]
        pos_c = jnp.concatenate([pos_t[:, 2 * b:2 * b + 1], pos_t[:, 2 * b + 1:2 * b + 2]], axis=0).astype(jnp.int32)
        start_c = q_iota[:, 0:1] - pos_c
        m_s[...] = jnp.full(m_s.shape, NEG, F32)
        l_s[...] = jnp.zeros(l_s.shape, F32)
        a_s[...] = jnp.zeros(a_s.shape, F32)

        def score(kp, carry):
            u = k_iota + (kp - piece) * PIECE
            bias = jnp.where((u <= q_iota) & (u >= start_c), 0.0, NEG)
            for g in range(4):
                r = slice(g * PIECE, (g + 1) * PIECE)
                s = lax.dot_general(qm[n, b, r, :], kk[n, kp], (((1,), (1,)), ((), ())), preferred_element_type=F32) + bias
                st[kp, r, :] = s
                m_s[r, :] = jnp.maximum(m_s[r, :], jnp.maximum(s[:, 0:128], s[:, 128:256]))
            return carry

        lax.fori_loop(0, piece + 1, score, 0)
        m_s[...] = jnp.broadcast_to(jnp.max(m_s[...], axis=-1, keepdims=True), m_s.shape)

        def expo(kp, carry):
            for g in range(4):
                r = slice(g * PIECE, (g + 1) * PIECE)
                e0 = jnp.exp(st[kp, r, 0:128] - m_s[r, :])
                e1 = jnp.exp(st[kp, r, 128:256] - m_s[r, :])
                st[kp, r, 0:128] = e0
                st[kp, r, 128:256] = e1
                l_s[r, :] += e0 + e1
            return carry

        lax.fori_loop(0, piece + 1, expo, 0)
        l_s[...] = jnp.broadcast_to(1.0 / jnp.sum(l_s[...], axis=-1, keepdims=True), l_s.shape)

        def mix(kp, carry):
            for g in range(4):
                r = slice(g * PIECE, (g + 1) * PIECE)
                p = jnp.concatenate([st[kp, r, 0:128] * l_s[r, :], st[kp, r, 128:256] * l_s[r, :]], axis=1).astype(BF16)
                a_s[r, :] += jnp.dot(p, vv[n, kp], preferred_element_type=F32)
            return carry

        lax.fori_loop(0, piece + 1, mix, 0)
        for a in range(2):
            even = a_s[2 * a * PIECE:(2 * a + 1) * PIECE, :]
            odd = a_s[(2 * a + 1) * PIECE:(2 * a + 2) * PIECE, :]
            o_all[tp, n, b * PIECE:(b + 1) * PIECE, a * 128:(a + 1) * 128] = jnp.where(low_head, even, odd).astype(BF16)

    def oc(direction, src, sub):
        part = o_all.at[src, sub // 2, pl.ds((sub % 2) * PIECE, PIECE)]
        return rcopy(part, part, o_ss.at[direction, src, sub], o_rs.at[src, sub], right if direction == 0 else left)

    for n in range(2):
        for b in range(2):
            attend(n, b)
            sub = 2 * n + b

            @pl.when(tp < TP - 1)
            def _():
                oc(0, tp, sub).start()

            @pl.when(tp > 0)
            def _():
                oc(1, tp, sub).start()

            if sub < 2:
                w_arrive(sub + 1)

    def product(j, rows, last):
        for t in range(4):
            cols = slice(t * 512, (t + 1) * 512)
            part = jnp.dot(o_all[j, 0, rows, :], wo_all[j, 0:256, cols], preferred_element_type=F32)
            part += jnp.dot(o_all[j, 1, rows, :], wo_all[j, 256:512, cols], preferred_element_type=F32)
            if last:
                y_ref[rows, cols] = (acc[rows, cols] + part).astype(BF16)
            else:
                acc[rows, cols] += part

    every = slice(0, ROWS)
    loads[5].wait()
    for t in range(4):
        cols = slice(t * 512, (t + 1) * 512)
        acc[:, cols] = xv[:, cols].astype(F32)
    product(tp, every, False)

    def o_step(s, sub):
        @pl.when(tp >= s)
        def _():
            oc(0, tp - s, sub).wait_recv()

        @pl.when((tp >= s) & (tp < TP - 1))
        def _():
            oc(0, tp - s, sub).start()

        @pl.when(tp + s < TP)
        def _():
            oc(1, tp + s, sub).wait_recv()

        @pl.when((tp + s < TP) & (tp > 0))
        def _():
            oc(1, tp + s, sub).start()

    for k in range(3):
        s = k + 1
        o_step(s, 0)
        w_step(k, 0)
        o_step(s, 1)
        w_step(k, 1)
        o_step(s, 2)
        w_step(k, 2)
        o_step(s, 3)
        for l in p_lanes:
            wforward(k, 0, l).wait_recv()
        product(order[k], every, k == 2)

    for b in range(2):
        kvc(0, b, mine[b], ynb).wait_send()
        kvc(1, b, mine[b], partner).wait_send()
        kvc(2, b, nb[b], partner).wait_send()
    for k in range(3):
        wz(k).wait_send()
        for i, dev in enumerate(peers + (partner,)):
            wsend(k, i, lane, dev).wait_send()
        for i in range(3):
            wforward(k, i, lanes[i]).wait_send()
    for s in range(0, TP):
        for sub in range(4):
            @pl.when((tp >= s) & (tp < TP - 1))
            def _():
                oc(0, tp - s, sub).wait_send()

            @pl.when((tp + s < TP) & (tp > 0))
            def _():
                oc(1, tp + s, sub).wait_send()


def layer(x, pos, gain, freq, wq, wk, wv, wo):
    hbm, vm = pl.BlockSpec(memory_space=pltpu.HBM), pl.BlockSpec(memory_space=pltpu.VMEM)
    sds = jax.ShapeDtypeStruct
    dma = pltpu.SemaphoreType.DMA
    return pl.pallas_call(
        layer_kernel,
        out_shape=(sds((ROWS, DM), BF16), sds((128, ROWS), BF16), sds((128, ROWS), BF16)),
        in_specs=[hbm, vm, vm, vm, hbm, hbm, hbm, hbm],
        out_specs=(vm, vm, vm),
        scratch_shapes=[
            pltpu.VMEM((ROWS, DM), BF16), pltpu.VMEM((DM, 512), BF16), pltpu.VMEM((DM, 256), BF16), pltpu.VMEM((ROWS, DM), BF16),
            pltpu.VMEM((ROWS, 128), F32), pltpu.VMEM((ROWS, 128), F32), pltpu.VMEM((8, PIECE, 256), BF16),
            pltpu.VMEM((2, 8, PIECE, 128), BF16), pltpu.VMEM((2, 8, PIECE, 128), BF16), pltpu.VMEM((2, 2, 4 * PIECE, 128), BF16),
            pltpu.VMEM((8, 4 * PIECE, PIECE), F32),
            pltpu.VMEM((4 * PIECE, 128), F32), pltpu.VMEM((4 * PIECE, 128), F32), pltpu.VMEM((4 * PIECE, 128), F32),
            pltpu.VMEM((TP, 2, ROWS, 256), BF16), pltpu.VMEM((TP, 512, DM), BF16), pltpu.VMEM((ROWS, DM), F32),
            dma((6,)), dma((3, 2)), dma((3, 2)), dma((3,)), dma((3, 4)), dma((3, 3)), dma((TP, 8)), dma((2, TP, 4)), dma((TP, 4)),
        ],
        compiler_params=pltpu.CompilerParams(collective_id=0, has_side_effects=True, vmem_limit_bytes=60 * 1024 * 1024),
        name='layer',
    )(x, pos, gain, freq, wq, wk, wv, wo)


def solution(mesh):
    def local_step(x, doc_id, pos, gain, wq, wk, wv, wo, inv_freq):
        y, kt, vt = layer(x, pos.reshape(4, BLK), gain.reshape(1, DM), inv_freq.reshape(1, 32), wq, wk, wv, wo)
        return y, kt.T.reshape(ROWS, 2, 64), vt.T.reshape(ROWS, 2, 64)

    row_spec = P(('dp', 'cp'))
    in_specs = (P(('dp', 'cp'), None), row_spec, row_spec, P(), P(None, 'tp'), P(None, 'tp'), P(None, 'tp'), P('tp', None), P())
    out_specs = (P(('dp', 'cp'), None), P(('dp', 'cp'), 'tp', None), P(('dp', 'cp'), 'tp', None))
    return jax.shard_map(local_step, mesh=mesh, in_specs=in_specs, out_specs=out_specs, check_vma=False)
```

```python
import jax
import jax.numpy as jnp
from jax import lax
from jax.experimental import pallas as pl
from jax.experimental.pallas import tpu as pltpu
from jax.sharding import PartitionSpec as P

MESH = pl.DeviceIdType.MESH
F32 = jnp.float32
BF16 = jnp.bfloat16
ROWS = 512
BLK = 128
PIECE = 256
DM = 2048
TP = 4
NEG = -1e30


def rcopy(src, dst, ssem, rsem, dev):
    return pltpu.make_async_remote_copy(src_ref=src, dst_ref=dst, send_sem=ssem, recv_sem=rsem, device_id=dev, device_id_type=MESH)


def layer_kernel(x_ref, pos_ref, gain_ref, freq_ref, wq_ref, wk_ref, wv_ref, wo_ref,
                 y_ref, kt_ref, vt_ref,
                 xv, wqv, wkv, h, cosv, sinv, kv_all, kk, vv, qm, st, m_s, l_s, a_s, o_all, wo_all, acc,
                 lsem, kv_ss, kv_rs, wz_ss, w_ss, f_ss, w_rs, o_ss, o_rs):
    dp, tp, cp = lax.axis_index('dp'), lax.axis_index('tp'), lax.axis_index('cp')
    y, c = cp // 2, cp % 2
    lane = dp * 4 + cp
    partner = (dp, tp, 2 * y + 1 - c)
    xnb = (1 - dp, tp, cp)
    ynb = (dp, tp, 2 * (1 - y) + c)
    dnb = (1 - dp, tp, 2 * (1 - y) + c)
    right, left = (dp, tp + 1, cp), (dp, tp - 1, cp)
    lanes = ((1 - dp) * 4 + cp, dp * 4 + 2 * (1 - y) + c, (1 - dp) * 4 + 2 * (1 - y) + c)
    peers = (xnb, ynb, dnb)
    p_lanes = tuple(l + 1 - 2 * c for l in (lane,) + lanes)
    mid, flip = tp * (3 - tp) // 2, tp // 2
    order = []
    for base in (1 + mid, 2 - 2 * mid, 3):
        order.append(base + flip * (3 - 2 * base))

    barrier = pltpu.get_barrier_semaphore()
    for dev in (partner,) + peers:
        pl.semaphore_signal(barrier, inc=1, device_id=dev, device_id_type=MESH)

    @pl.when(tp < TP - 1)
    def _():
        pl.semaphore_signal(barrier, inc=1, device_id=right, device_id_type=MESH)

    @pl.when(tp > 0)
    def _():
        pl.semaphore_signal(barrier, inc=1, device_id=left, device_id_type=MESH)

    loads = []
    for b in range(2):
        rows = pl.ds(b * PIECE, PIECE)
        loads.append(pltpu.make_async_copy(x_ref.at[rows], xv.at[rows], lsem.at[b]))
    loads.append(pltpu.make_async_copy(wk_ref, wkv.at[:, pl.ds(0, 128)], lsem.at[2]))
    loads.append(pltpu.make_async_copy(wv_ref, wkv.at[:, pl.ds(128, 128)], lsem.at[3]))
    loads.append(pltpu.make_async_copy(wq_ref, wqv, lsem.at[4]))
    loads.append(pltpu.make_async_copy(wo_ref, wo_all.at[tp], lsem.at[5]))
    for i in (5, 0, 2, 3, 1, 4):
        loads[i].start()

    lane_i = lax.broadcasted_iota(jnp.int32, (BLK, 128), 1)
    pos_t = jnp.concatenate([pos_ref[...].astype(F32), jnp.zeros((4, BLK), F32)], axis=0).T
    freq = jnp.concatenate([freq_ref[...]] * 4, axis=1)
    pos_l = jnp.zeros((BLK, 128), F32)
    for b in range(4):
        pos_l = jnp.where(lane_i // 32 == b, pos_t[:, b:b + 1], pos_l)
    ang = pos_l * freq
    tables = (jnp.cos(ang), jnp.sin(ang))
    low32 = (lane_i % 64) < 32
    for b in range(4):
        for ref, tab in zip((cosv, sinv), tables):
            t = jnp.where(lane_i // 32 == b, tab, 0.0)
            t = t + pltpu.roll(t, 32, 1)
            t = t + pltpu.roll(t, 64, 1)
            if ref is sinv:
                t = jnp.where(low32, -t, t)
            ref[b * BLK:(b + 1) * BLK, :] = t

    pl.semaphore_wait(barrier, 5 + mid)

    def slot(j, l, half):
        return wo_all.at[j, pl.ds(l * 64 + half * 32, 32)]

    def wz(direction, j, half):
        part = slot(j, lane, half)
        return rcopy(part, part, wz_ss.at[direction, j, half], w_rs.at[j, lane, half], right if direction == 0 else left)

    def wsend(j, half, i, l, dev):
        part = slot(j, l, half)
        return rcopy(part, part, w_ss.at[j, half, i], w_rs.at[j, l, half], dev)

    def wforward(j, half, i, l):
        part = slot(j, l, half)
        return rcopy(part, part, f_ss.at[j, half, i], w_rs.at[j, l, half], partner)

    def wz_step(s, half):
        @pl.when(tp >= s)
        def _():
            wz(0, tp - s, half).wait_recv()

        @pl.when((tp >= s) & (tp < TP - 1))
        def _():
            wz(0, tp - s, half).start()

        @pl.when(tp >= s)
        def _():
            for i, dev in enumerate(peers + (partner,)):
                wsend(tp - s, half, i, lane, dev).start()

        @pl.when(tp + s < TP)
        def _():
            wz(1, tp + s, half).wait_recv()

        @pl.when((tp + s < TP) & (tp > 0))
        def _():
            wz(1, tp + s, half).start()

        @pl.when(tp + s < TP)
        def _():
            for i, dev in enumerate(peers + (partner,)):
                wsend(tp + s, half, i, lane, dev).start()

    loads[5].wait()

    @pl.when(tp < TP - 1)
    def _():
        wz(0, tp, 0).start()
        wz(0, tp, 1).start()

    @pl.when(tp > 0)
    def _():
        wz(1, tp, 0).start()
        wz(1, tp, 1).start()

    def w_step(k, i):
        for half in range(2):
            wsend(order[k], half, i, lanes[i], peers[i]).wait_recv()
            wforward(order[k], half, i, lanes[i]).start()

    def w_ready(k):
        for l in p_lanes:
            for half in range(2):
                wforward(order[k], half, 0, l).wait_recv()

    def norm(b):
        rows = pl.ds(b * PIECE, PIECE)
        xf = xv[rows, :].astype(F32)
        inv = lax.rsqrt(jnp.mean(xf * xf, axis=-1, keepdims=True) + 1e-5)
        h[rows, :] = (xf * inv * gain_ref[...]).astype(BF16)

    low = lax.broadcasted_iota(jnp.int32, (PIECE, 128), 1)
    low_head = low < 64
    low_half = (low % 64) < 32

    def rotate(t, rows):
        turned = jnp.where(low_half, pltpu.roll(t, 96, 1), pltpu.roll(t, 32, 1))
        return t * cosv[rows, :] + turned * sinv[rows, :]

    mine = (cp, 7 - cp)
    nb_cp, pt_cp, pd_cp = 2 * (1 - y) + c, 2 * y + 1 - c, 2 * (1 - y) + 1 - c
    nb, pt, pd = (nb_cp, 7 - nb_cp), (pt_cp, 7 - pt_cp), (pd_cp, 7 - pd_cp)

    def kvc(kind, half, piece, dev):
        return rcopy(kv_all.at[piece], kv_all.at[piece], kv_ss.at[kind, half], kv_rs.at[kind, half], dev)

    for b in range(2):
        rows = slice(b * PIECE, (b + 1) * PIECE)
        loads[b].wait()
        norm(b)
        if b == 0:
            loads[2].wait()
            loads[3].wait()
        kv = jnp.dot(h[rows, :], wkv[...], preferred_element_type=F32).astype(BF16)
        k_rot = rotate(kv[:, 0:128].astype(F32), rows).astype(BF16)
        kv_all[mine[b], :, 0:128] = k_rot
        kv_all[mine[b], :, 128:256] = kv[:, 128:256]
        kt_ref[:, rows] = k_rot.astype(F32).T.astype(BF16)
        vt_ref[:, rows] = kv[:, 128:256].astype(F32).T.astype(BF16)
        kvc(0, b, mine[b], ynb).start()
        kvc(1, b, mine[b], partner).start()

    loads[4].wait()
    for b in range(2):
        rows = slice(b * PIECE, (b + 1) * PIECE)
        qf = jnp.dot(h[rows, :], wqv[...], preferred_element_type=F32).astype(BF16).astype(F32)
        for g in range(4):
            q = rotate(qf[:, g * 128:(g + 1) * 128], rows).astype(BF16)
            q = (q.astype(F32) * 0.125).astype(BF16)
            zero = jnp.zeros_like(q)
            at = (g % 2) * 2 * PIECE
            qm[g // 2, b, at:at + PIECE, :] = jnp.where(low_head, q, zero)
            qm[g // 2, b, at + PIECE:at + 2 * PIECE, :] = jnp.where(low_head, zero, q)

    def double(piece):
        for i, ref in enumerate((kk, vv)):
            t = kv_all[piece, :, i * 128:(i + 1) * 128]
            r = pltpu.roll(t.astype(F32), 64, 1).astype(BF16)
            ref[0, piece] = jnp.where(low_head, t, r)
            ref[1, piece] = jnp.where(low_head, r, t)

    wz_step(1, 0)
    double(mine[0])
    double(mine[1])
    kvc(0, 0, nb[0], ynb).wait_recv()
    kvc(2, 0, nb[0], partner).start()
    double(nb[0])
    wz_step(1, 1)
    kvc(1, 0, pt[0], partner).wait_recv()
    double(pt[0])
    kvc(1, 1, pt[1], partner).wait_recv()
    double(pt[1])
    kvc(0, 1, nb[1], ynb).wait_recv()
    kvc(2, 1, nb[1], partner).start()
    double(nb[1])
    kvc(2, 0, pd[0], partner).wait_recv()
    double(pd[0])
    kvc(2, 1, pd[1], partner).wait_recv()
    double(pd[1])
    wz_step(2, 0)

    q_iota = lax.broadcasted_iota(jnp.int32, (PIECE, PIECE), 0)
    k_iota = lax.broadcasted_iota(jnp.int32, (PIECE, PIECE), 1)

    def attend(n, b, poll):
        piece = mine[b]
        pos_c = jnp.concatenate([pos_t[:, 2 * b:2 * b + 1], pos_t[:, 2 * b + 1:2 * b + 2]], axis=0).astype(jnp.int32)
        start_c = q_iota[:, 0:1] - pos_c
        m_s[...] = jnp.full(m_s.shape, NEG, F32)
        l_s[...] = jnp.zeros(l_s.shape, F32)
        a_s[...] = jnp.zeros(a_s.shape, F32)

        def score(kp, carry):
            u = k_iota + (kp - piece) * PIECE
            bias = jnp.where((u <= q_iota) & (u >= start_c), 0.0, NEG)
            for g in range(4):
                r = slice(g * PIECE, (g + 1) * PIECE)
                s = lax.dot_general(qm[n, b, r, :], kk[n, kp], (((1,), (1,)), ((), ())), preferred_element_type=F32) + bias
                st[kp, r, :] = s
                m_s[r, :] = jnp.maximum(m_s[r, :], jnp.maximum(s[:, 0:128], s[:, 128:256]))
            return carry

        lax.fori_loop(0, piece + 1, score, 0)
        poll()
        m_s[...] = jnp.broadcast_to(jnp.max(m_s[...], axis=-1, keepdims=True), m_s.shape)

        def expo(kp, carry):
            for g in range(4):
                r = slice(g * PIECE, (g + 1) * PIECE)
                e0 = jnp.exp(st[kp, r, 0:128] - m_s[r, :])
                e1 = jnp.exp(st[kp, r, 128:256] - m_s[r, :])
                st[kp, r, 0:128] = e0
                st[kp, r, 128:256] = e1
                l_s[r, :] += e0 + e1
            return carry

        lax.fori_loop(0, piece + 1, expo, 0)
        l_s[...] = jnp.broadcast_to(1.0 / jnp.sum(l_s[...], axis=-1, keepdims=True), l_s.shape)

        def mix(kp, carry):
            for g in range(4):
                r = slice(g * PIECE, (g + 1) * PIECE)
                p = jnp.concatenate([st[kp, r, 0:128] * l_s[r, :], st[kp, r, 128:256] * l_s[r, :]], axis=1).astype(BF16)
                a_s[r, :] += jnp.dot(p, vv[n, kp], preferred_element_type=F32)
            return carry

        lax.fori_loop(0, piece + 1, mix, 0)
        for a in range(2):
            even = a_s[2 * a * PIECE:(2 * a + 1) * PIECE, :]
            odd = a_s[(2 * a + 1) * PIECE:(2 * a + 2) * PIECE, :]
            o_all[tp, n, b * PIECE:(b + 1) * PIECE, a * 128:(a + 1) * 128] = jnp.where(low_head, even, odd).astype(BF16)

    def oc(direction, src, sub):
        part = o_all.at[src, sub // 2, pl.ds((sub % 2) * PIECE, PIECE)]
        return rcopy(part, part, o_ss.at[direction, src, sub], o_rs.at[src, sub], right if direction == 0 else left)

    def o_step(s, sub):
        @pl.when(tp >= s)
        def _():
            oc(0, tp - s, sub).wait_recv()

        @pl.when((tp >= s) & (tp < TP - 1))
        def _():
            oc(0, tp - s, sub).start()

        @pl.when(tp + s < TP)
        def _():
            oc(1, tp + s, sub).wait_recv()

        @pl.when((tp + s < TP) & (tp > 0))
        def _():
            oc(1, tp + s, sub).start()

    def o_send(sub):
        @pl.when(tp < TP - 1)
        def _():
            oc(0, tp, sub).start()

        @pl.when(tp > 0)
        def _():
            oc(1, tp, sub).start()

    def nothing():
        pass

    attend(0, 0, lambda: wz_step(2, 1))
    o_send(0)
    attend(0, 1, nothing)
    o_send(1)
    wz_step(3, 0)
    wz_step(3, 1)
    attend(1, 0, nothing)
    o_send(2)
    o_step(1, 0)
    attend(1, 1, lambda: o_step(1, 1))
    o_send(3)

    def product(j):
        for t in range(4):
            cols = slice(t * 512, (t + 1) * 512)
            part = jnp.dot(o_all[j, 0], wo_all[j, 0:256, cols], preferred_element_type=F32)
            part += jnp.dot(o_all[j, 1], wo_all[j, 256:512, cols], preferred_element_type=F32)
            acc[:, cols] += part

    for t in range(4):
        cols = slice(t * 512, (t + 1) * 512)
        acc[:, cols] = xv[:, cols].astype(F32)
    product(tp)

    for i in range(3):
        w_step(0, i)
    o_step(1, 2)
    o_step(1, 3)
    w_ready(0)
    product(order[0])
    o_step(2, 0)
    o_step(2, 1)
    for i in range(3):
        w_step(1, i)
    o_step(2, 2)
    o_step(2, 3)
    w_ready(1)
    product(order[1])
    for i in range(3):
        w_step(2, i)
    o_step(3, 0)
    w_ready(2)
    for sub in range(4):
        n, b = sub // 2, sub % 2
        rows = slice(b * PIECE, (b + 1) * PIECE)
        if sub > 0:
            o_step(3, sub)
        for t in range(4):
            cols = slice(t * 512, (t + 1) * 512)
            part = jnp.dot(o_all[order[2], n, rows, :], wo_all[order[2], n * 256:(n + 1) * 256, cols], preferred_element_type=F32)
            if n == 0:
                acc[rows, cols] += part
            else:
                y_ref[rows, cols] = (acc[rows, cols] + part).astype(BF16)

    for b in range(2):
        kvc(0, b, mine[b], ynb).wait_send()
        kvc(1, b, mine[b], partner).wait_send()
        kvc(2, b, nb[b], partner).wait_send()
    for j in order:
        for half in range(2):
            for i, dev in enumerate(peers + (partner,)):
                wsend(j, half, i, lane, dev).wait_send()
            for i in range(3):
                wforward(j, half, i, lanes[i]).wait_send()
    for s in range(0, TP):
        for half in range(2):
            @pl.when((tp >= s) & (tp < TP - 1))
            def _():
                wz(0, tp - s, half).wait_send()

            @pl.when((tp + s < TP) & (tp > 0))
            def _():
                wz(1, tp + s, half).wait_send()
    for s in range(0, TP):
        for sub in range(4):
            @pl.when((tp >= s) & (tp < TP - 1))
            def _():
                oc(0, tp - s, sub).wait_send()

            @pl.when((tp + s < TP) & (tp > 0))
            def _():
                oc(1, tp + s, sub).wait_send()


def layer(x, pos, gain, freq, wq, wk, wv, wo):
    hbm, vm = pl.BlockSpec(memory_space=pltpu.HBM), pl.BlockSpec(memory_space=pltpu.VMEM)
    dma = pltpu.SemaphoreType.DMA
    return pl.pallas_call(
        layer_kernel,
        out_shape=(pltpu.VMEM((ROWS, DM), BF16), pltpu.VMEM((128, ROWS), BF16), pltpu.VMEM((128, ROWS), BF16)),
        in_specs=[hbm, vm, vm, vm, hbm, hbm, hbm, hbm],
        out_specs=(vm, vm, vm),
        scratch_shapes=[
            pltpu.VMEM((ROWS, DM), BF16), pltpu.VMEM((DM, 512), BF16), pltpu.VMEM((DM, 256), BF16), pltpu.VMEM((ROWS, DM), BF16),
            pltpu.VMEM((ROWS, 128), F32), pltpu.VMEM((ROWS, 128), F32), pltpu.VMEM((8, PIECE, 256), BF16),
            pltpu.VMEM((2, 8, PIECE, 128), BF16), pltpu.VMEM((2, 8, PIECE, 128), BF16), pltpu.VMEM((2, 2, 4 * PIECE, 128), BF16),
            pltpu.VMEM((8, 4 * PIECE, PIECE), F32),
            pltpu.VMEM((4 * PIECE, 128), F32), pltpu.VMEM((4 * PIECE, 128), F32), pltpu.VMEM((4 * PIECE, 128), F32),
            pltpu.VMEM((TP, 2, ROWS, 256), BF16), pltpu.VMEM((TP, 512, DM), BF16), pltpu.VMEM((ROWS, DM), F32),
            dma((6,)), dma((3, 2)), dma((3, 2)), dma((2, TP, 2)), dma((TP, 2, 4)), dma((TP, 2, 3)), dma((TP, 8, 2)), dma((2, TP, 4)), dma((TP, 4)),
        ],
        compiler_params=pltpu.CompilerParams(collective_id=0, has_side_effects=True, vmem_limit_bytes=60 * 1024 * 1024),
        name='layer',
    )(x, pos, gain, freq, wq, wk, wv, wo)


def solution(mesh):
    def local_step(x, doc_id, pos, gain, wq, wk, wv, wo, inv_freq):
        y, kt, vt = layer(x, pos.reshape(4, BLK), gain.reshape(1, DM), inv_freq.reshape(1, 32), wq, wk, wv, wo)
        return y, kt.T.reshape(ROWS, 2, 64), vt.T.reshape(ROWS, 2, 64)

    row_spec = P(('dp', 'cp'))
    in_specs = (P(('dp', 'cp'), None), row_spec, row_spec, P(), P(None, 'tp'), P(None, 'tp'), P(None, 'tp'), P('tp', None), P())
    out_specs = (P(('dp', 'cp'), None), P(('dp', 'cp'), 'tp', None), P(('dp', 'cp'), 'tp', None))
    return jax.shard_map(local_step, mesh=mesh, in_specs=in_specs, out_specs=out_specs, check_vma=False)
```

```python
import jax
import jax.numpy as jnp
from jax import lax
from jax.experimental import pallas as pl
from jax.experimental.pallas import tpu as pltpu
from jax.sharding import PartitionSpec as P

MESH = pl.DeviceIdType.MESH
F32 = jnp.float32
BF16 = jnp.bfloat16
ROWS = 512
BLK = 128
PIECE = 256
DM = 2048
TP = 4
NEG = -1e30


def rcopy(src, dst, ssem, rsem, dev):
    return pltpu.make_async_remote_copy(src_ref=src, dst_ref=dst, send_sem=ssem, recv_sem=rsem, device_id=dev, device_id_type=MESH)


def layer_kernel(x_ref, pos_ref, gain_ref, freq_ref, wq_ref, wk_ref, wv_ref, wo_ref,
                 ya_ref, accb_ref, olast_ref, wlast_ref, kt_ref, vt_ref,
                 posv, gainv, freqv, xv, wqv, wkv, h, cosv, sinv, kv_all, kk, vv, qm, st, m_s, l_s, a_s, o_all, wo_all, acca,
                 lsem, kv_ss, kv_rs, wz_ss, w_ss, f_ss, w_rs, o_ss, o_rs):
    dp, tp, cp = lax.axis_index('dp'), lax.axis_index('tp'), lax.axis_index('cp')
    y, c = cp // 2, cp % 2
    lane = dp * 4 + cp
    partner = (dp, tp, 2 * y + 1 - c)
    xnb = (1 - dp, tp, cp)
    ynb = (dp, tp, 2 * (1 - y) + c)
    dnb = (1 - dp, tp, 2 * (1 - y) + c)
    right, left = (dp, tp + 1, cp), (dp, tp - 1, cp)
    lanes = ((1 - dp) * 4 + cp, dp * 4 + 2 * (1 - y) + c, (1 - dp) * 4 + 2 * (1 - y) + c)
    peers = (xnb, ynb, dnb)
    p_lanes = tuple(l + 1 - 2 * c for l in (lane,) + lanes)
    mid, flip = tp * (3 - tp) // 2, tp // 2
    order = []
    for base in (1 + mid, 2 - 2 * mid, 3):
        order.append(base + flip * (3 - 2 * base))

    barrier = pltpu.get_barrier_semaphore()
    for dev in (partner,) + peers:
        pl.semaphore_signal(barrier, inc=1, device_id=dev, device_id_type=MESH)

    @pl.when(tp < TP - 1)
    def _():
        pl.semaphore_signal(barrier, inc=1, device_id=right, device_id_type=MESH)

    @pl.when(tp > 0)
    def _():
        pl.semaphore_signal(barrier, inc=1, device_id=left, device_id_type=MESH)

    loads = []
    for b in range(2):
        rows = pl.ds(b * PIECE, PIECE)
        loads.append(pltpu.make_async_copy(x_ref.at[rows], xv.at[rows], lsem.at[b]))
    loads.append(pltpu.make_async_copy(wk_ref, wkv.at[:, pl.ds(0, 128)], lsem.at[2]))
    loads.append(pltpu.make_async_copy(wv_ref, wkv.at[:, pl.ds(128, 128)], lsem.at[3]))
    loads.append(pltpu.make_async_copy(wq_ref, wqv, lsem.at[4]))
    loads.append(pltpu.make_async_copy(wo_ref, wo_all.at[tp], lsem.at[5]))
    for i, (src, dst) in enumerate(((pos_ref, posv), (freq_ref, freqv), (gain_ref, gainv))):
        loads.append(pltpu.make_async_copy(src, dst, lsem.at[6 + i]))
    for i in (6, 7, 5, 8, 0, 2, 3, 1, 4):
        loads[i].start()
    loads[6].wait()
    loads[7].wait()

    lane_i = lax.broadcasted_iota(jnp.int32, (BLK, 128), 1)
    pos_t = jnp.concatenate([posv[...].astype(F32), jnp.zeros((4, BLK), F32)], axis=0).T
    freq = jnp.concatenate([freqv[...]] * 4, axis=1)
    pos_l = jnp.zeros((BLK, 128), F32)
    for b in range(4):
        pos_l = jnp.where(lane_i // 32 == b, pos_t[:, b:b + 1], pos_l)
    ang = pos_l * freq
    tables = (jnp.cos(ang), jnp.sin(ang))
    low32 = (lane_i % 64) < 32
    for b in range(4):
        for ref, tab in zip((cosv, sinv), tables):
            t = jnp.where(lane_i // 32 == b, tab, 0.0)
            t = t + pltpu.roll(t, 32, 1)
            t = t + pltpu.roll(t, 64, 1)
            if ref is sinv:
                t = jnp.where(low32, -t, t)
            ref[b * BLK:(b + 1) * BLK, :] = t

    pl.semaphore_wait(barrier, 5 + mid)

    def slot(j, l, half):
        return wo_all.at[j, pl.ds(l * 64 + half * 32, 32)]

    def wz(direction, j, half):
        part = slot(j, lane, half)
        return rcopy(part, part, wz_ss.at[direction, j, half], w_rs.at[j, lane, half], right if direction == 0 else left)

    def wsend(j, half, i, l, dev):
        part = slot(j, l, half)
        return rcopy(part, part, w_ss.at[j, half, i], w_rs.at[j, l, half], dev)

    def wforward(j, half, i, l):
        part = slot(j, l, half)
        return rcopy(part, part, f_ss.at[j, half, i], w_rs.at[j, l, half], partner)

    def wz_step(s, half):
        @pl.when(tp >= s)
        def _():
            wz(0, tp - s, half).wait_recv()

        @pl.when((tp >= s) & (tp < TP - 1))
        def _():
            wz(0, tp - s, half).start()

        @pl.when(tp >= s)
        def _():
            for i, dev in enumerate(peers + (partner,)):
                wsend(tp - s, half, i, lane, dev).start()

        @pl.when(tp + s < TP)
        def _():
            wz(1, tp + s, half).wait_recv()

        @pl.when((tp + s < TP) & (tp > 0))
        def _():
            wz(1, tp + s, half).start()

        @pl.when(tp + s < TP)
        def _():
            for i, dev in enumerate(peers + (partner,)):
                wsend(tp + s, half, i, lane, dev).start()

    loads[5].wait()

    @pl.when(tp < TP - 1)
    def _():
        wz(0, tp, 0).start()
        wz(0, tp, 1).start()

    @pl.when(tp > 0)
    def _():
        wz(1, tp, 0).start()
        wz(1, tp, 1).start()

    def w_step(k, i):
        for half in range(2):
            wsend(order[k], half, i, lanes[i], peers[i]).wait_recv()
            wforward(order[k], half, i, lanes[i]).start()

    def w_ready(k):
        for l in p_lanes:
            for half in range(2):
                wforward(order[k], half, 0, l).wait_recv()

    def norm(b):
        rows = pl.ds(b * PIECE, PIECE)
        xf = xv[rows, :].astype(F32)
        inv = lax.rsqrt(jnp.mean(xf * xf, axis=-1, keepdims=True) + 1e-5)
        h[rows, :] = (xf * inv * gainv[...]).astype(BF16)

    low = lax.broadcasted_iota(jnp.int32, (PIECE, 128), 1)
    low_head = low < 64
    low_half = (low % 64) < 32

    def rotate(t, rows):
        turned = jnp.where(low_half, pltpu.roll(t, 96, 1), pltpu.roll(t, 32, 1))
        return t * cosv[rows, :] + turned * sinv[rows, :]

    mine = (cp, 7 - cp)
    nb_cp, pt_cp, pd_cp = 2 * (1 - y) + c, 2 * y + 1 - c, 2 * (1 - y) + 1 - c
    nb, pt, pd = (nb_cp, 7 - nb_cp), (pt_cp, 7 - pt_cp), (pd_cp, 7 - pd_cp)

    def kvc(kind, half, piece, dev):
        return rcopy(kv_all.at[piece], kv_all.at[piece], kv_ss.at[kind, half], kv_rs.at[kind, half], dev)

    for b in range(2):
        rows = slice(b * PIECE, (b + 1) * PIECE)
        if b == 0:
            loads[8].wait()
        loads[b].wait()
        norm(b)
        if b == 0:
            loads[2].wait()
            loads[3].wait()
        kv = jnp.dot(h[rows, :], wkv[...], preferred_element_type=F32).astype(BF16)
        k_rot = rotate(kv[:, 0:128].astype(F32), rows).astype(BF16)
        kv_all[mine[b], :, 0:128] = k_rot
        kv_all[mine[b], :, 128:256] = kv[:, 128:256]
        kt_ref[:, rows] = k_rot.astype(F32).T.astype(BF16)
        vt_ref[:, rows] = kv[:, 128:256].astype(F32).T.astype(BF16)
        kvc(0, b, mine[b], ynb).start()
        kvc(1, b, mine[b], partner).start()

    loads[4].wait()
    for b in range(2):
        rows = slice(b * PIECE, (b + 1) * PIECE)
        qf = jnp.dot(h[rows, :], wqv[...], preferred_element_type=F32).astype(BF16).astype(F32)
        for g in range(4):
            q = rotate(qf[:, g * 128:(g + 1) * 128], rows).astype(BF16)
            q = (q.astype(F32) * 0.125).astype(BF16)
            zero = jnp.zeros_like(q)
            at = (g % 2) * 2 * PIECE
            qm[g // 2, b, at:at + PIECE, :] = jnp.where(low_head, q, zero)
            qm[g // 2, b, at + PIECE:at + 2 * PIECE, :] = jnp.where(low_head, zero, q)

    def double(piece):
        for i, ref in enumerate((kk, vv)):
            t = kv_all[piece, :, i * 128:(i + 1) * 128]
            r = pltpu.roll(t.astype(F32), 64, 1).astype(BF16)
            ref[0, piece] = jnp.where(low_head, t, r)
            ref[1, piece] = jnp.where(low_head, r, t)

    wz_step(1, 0)
    double(mine[0])
    double(mine[1])
    kvc(0, 0, nb[0], ynb).wait_recv()
    kvc(2, 0, nb[0], partner).start()
    double(nb[0])
    wz_step(1, 1)
    kvc(1, 0, pt[0], partner).wait_recv()
    double(pt[0])
    kvc(1, 1, pt[1], partner).wait_recv()
    double(pt[1])
    kvc(0, 1, nb[1], ynb).wait_recv()
    kvc(2, 1, nb[1], partner).start()
    double(nb[1])
    kvc(2, 0, pd[0], partner).wait_recv()
    double(pd[0])
    kvc(2, 1, pd[1], partner).wait_recv()
    double(pd[1])
    wz_step(2, 0)

    q_iota = lax.broadcasted_iota(jnp.int32, (PIECE, PIECE), 0)
    k_iota = lax.broadcasted_iota(jnp.int32, (PIECE, PIECE), 1)

    def attend(n, b, poll, poll2=lambda: None):
        piece = mine[b]
        pos_c = jnp.concatenate([pos_t[:, 2 * b:2 * b + 1], pos_t[:, 2 * b + 1:2 * b + 2]], axis=0).astype(jnp.int32)
        start_c = q_iota[:, 0:1] - pos_c
        m_s[...] = jnp.full(m_s.shape, NEG, F32)
        l_s[...] = jnp.zeros(l_s.shape, F32)
        a_s[...] = jnp.zeros(a_s.shape, F32)

        def score(kp, carry):
            u = k_iota + (kp - piece) * PIECE
            bias = jnp.where((u <= q_iota) & (u >= start_c), 0.0, NEG)
            for g in range(4):
                r = slice(g * PIECE, (g + 1) * PIECE)
                s = lax.dot_general(qm[n, b, r, :], kk[n, kp], (((1,), (1,)), ((), ())), preferred_element_type=F32) + bias
                st[kp, r, :] = s
                m_s[r, :] = jnp.maximum(m_s[r, :], jnp.maximum(s[:, 0:128], s[:, 128:256]))
            return carry

        lax.fori_loop(0, piece + 1, score, 0)
        poll()
        m_s[...] = jnp.broadcast_to(jnp.max(m_s[...], axis=-1, keepdims=True), m_s.shape)

        def expo(kp, carry):
            for g in range(4):
                r = slice(g * PIECE, (g + 1) * PIECE)
                e0 = jnp.exp(st[kp, r, 0:128] - m_s[r, :])
                e1 = jnp.exp(st[kp, r, 128:256] - m_s[r, :])
                st[kp, r, 0:128] = e0
                st[kp, r, 128:256] = e1
                l_s[r, :] += e0 + e1
            return carry

        lax.fori_loop(0, piece + 1, expo, 0)
        poll2()
        l_s[...] = jnp.broadcast_to(1.0 / jnp.sum(l_s[...], axis=-1, keepdims=True), l_s.shape)

        def mix(kp, carry):
            for g in range(4):
                r = slice(g * PIECE, (g + 1) * PIECE)
                p = jnp.concatenate([st[kp, r, 0:128] * l_s[r, :], st[kp, r, 128:256] * l_s[r, :]], axis=1).astype(BF16)
                a_s[r, :] += jnp.dot(p, vv[n, kp], preferred_element_type=F32)
            return carry

        lax.fori_loop(0, piece + 1, mix, 0)
        for a in range(2):
            even = a_s[2 * a * PIECE:(2 * a + 1) * PIECE, :]
            odd = a_s[(2 * a + 1) * PIECE:(2 * a + 2) * PIECE, :]
            o_all[tp, n, b * PIECE:(b + 1) * PIECE, a * 128:(a + 1) * 128] = jnp.where(low_head, even, odd).astype(BF16)

    def oc(direction, src, sub):
        part = o_all.at[src, sub % 2, pl.ds((sub // 2) * PIECE, PIECE)]
        return rcopy(part, part, o_ss.at[direction, src, sub], o_rs.at[src, sub], right if direction == 0 else left)

    def o_step(s, sub):
        @pl.when(tp >= s)
        def _():
            oc(0, tp - s, sub).wait_recv()

        @pl.when((tp >= s) & (tp < TP - 1))
        def _():
            oc(0, tp - s, sub).start()

        @pl.when(tp + s < TP)
        def _():
            oc(1, tp + s, sub).wait_recv()

        @pl.when((tp + s < TP) & (tp > 0))
        def _():
            oc(1, tp + s, sub).start()

    def o_send(sub):
        @pl.when(tp < TP - 1)
        def _():
            oc(0, tp, sub).start()

        @pl.when(tp > 0)
        def _():
            oc(1, tp, sub).start()

    def nothing():
        pass

    attend(0, 0, nothing, lambda: wz_step(2, 1))
    o_send(0)
    attend(1, 0, nothing)
    o_send(1)
    wz_step(3, 0)
    attend(0, 1, nothing, lambda: wz_step(3, 1))
    o_send(2)
    attend(1, 1, lambda: o_step(1, 0))
    o_send(3)
    o_step(1, 1)

    accs = (acca, accb_ref)

    def product(j):
        for b in range(2):
            rows = slice(b * PIECE, (b + 1) * PIECE)
            for t in range(4):
                cols = slice(t * 512, (t + 1) * 512)
                part = jnp.dot(o_all[j, 0, rows, :], wo_all[j, 0:256, cols], preferred_element_type=F32)
                part += jnp.dot(o_all[j, 1, rows, :], wo_all[j, 256:512, cols], preferred_element_type=F32)
                accs[b][:, cols] += part

    for b in range(2):
        rows = slice(b * PIECE, (b + 1) * PIECE)
        accs[b][...] = xv[rows, :].astype(F32)
    product(tp)

    for i in range(3):
        w_step(0, i)
    o_step(1, 2)
    o_step(1, 3)
    w_ready(0)
    product(order[0])
    o_step(2, 0)
    o_step(2, 1)
    for i in range(3):
        w_step(1, i)
    o_step(2, 2)
    o_step(2, 3)
    w_ready(1)
    product(order[1])
    for i in range(3):
        w_step(2, i)
    o_step(3, 0)
    w_ready(2)
    far = order[2]
    w_out = pltpu.make_async_copy(wo_all.at[far, pl.ds(256, 256)], wlast_ref, lsem.at[9])
    w_out.start()
    o_step(3, 1)
    for t in range(4):
        cols = slice(t * 512, (t + 1) * 512)
        part = jnp.dot(o_all[far, 0, 0:PIECE, :], wo_all[far, 0:256, cols], preferred_element_type=F32)
        part += jnp.dot(o_all[far, 1, 0:PIECE, :], wo_all[far, 256:512, cols], preferred_element_type=F32)
        ya_ref[:, cols] = (acca[:, cols] + part).astype(BF16)
    o_step(3, 2)
    for t in range(4):
        cols = slice(t * 512, (t + 1) * 512)
        accb_ref[:, cols] += jnp.dot(o_all[far, 0, PIECE:ROWS, :], wo_all[far, 0:256, cols], preferred_element_type=F32)

    for b in range(2):
        kvc(0, b, mine[b], ynb).wait_send()
        kvc(1, b, mine[b], partner).wait_send()
        kvc(2, b, nb[b], partner).wait_send()
    for j in order:
        for half in range(2):
            for i, dev in enumerate(peers + (partner,)):
                wsend(j, half, i, lane, dev).wait_send()
            for i in range(3):
                wforward(j, half, i, lanes[i]).wait_send()
    for s in range(0, TP):
        for half in range(2):
            @pl.when((tp >= s) & (tp < TP - 1))
            def _():
                wz(0, tp - s, half).wait_send()

            @pl.when((tp + s < TP) & (tp > 0))
            def _():
                wz(1, tp + s, half).wait_send()
    for s in range(0, TP):
        for sub in range(4):
            @pl.when((tp >= s) & (tp < TP - 1))
            def _():
                oc(0, tp - s, sub).wait_send()

            @pl.when((tp + s < TP) & (tp > 0))
            def _():
                oc(1, tp + s, sub).wait_send()
    w_out.wait()
    o_step(3, 3)
    olast_ref[...] = o_all[far, 1, PIECE:ROWS, :]


def layer(x, pos, gain, freq, wq, wk, wv, wo):
    hbm, vm = pl.BlockSpec(memory_space=pltpu.HBM), pl.BlockSpec(memory_space=pltpu.VMEM)
    dma = pltpu.SemaphoreType.DMA
    return pl.pallas_call(
        layer_kernel,
        out_shape=(pltpu.VMEM((PIECE, DM), BF16), pltpu.VMEM((PIECE, DM), F32), pltpu.VMEM((PIECE, 256), BF16), pltpu.VMEM((256, DM), BF16), pltpu.VMEM((128, ROWS), BF16), pltpu.VMEM((128, ROWS), BF16)),
        in_specs=[hbm] * 8,
        out_specs=(vm,) * 6,
        scratch_shapes=[
            pltpu.VMEM((4, BLK), jnp.int32), pltpu.VMEM((1, DM), F32), pltpu.VMEM((1, 32), F32),
            pltpu.VMEM((ROWS, DM), BF16), pltpu.VMEM((DM, 512), BF16), pltpu.VMEM((DM, 256), BF16), pltpu.VMEM((ROWS, DM), BF16),
            pltpu.VMEM((ROWS, 128), F32), pltpu.VMEM((ROWS, 128), F32), pltpu.VMEM((8, PIECE, 256), BF16),
            pltpu.VMEM((2, 8, PIECE, 128), BF16), pltpu.VMEM((2, 8, PIECE, 128), BF16), pltpu.VMEM((2, 2, 4 * PIECE, 128), BF16),
            pltpu.VMEM((8, 4 * PIECE, PIECE), F32),
            pltpu.VMEM((4 * PIECE, 128), F32), pltpu.VMEM((4 * PIECE, 128), F32), pltpu.VMEM((4 * PIECE, 128), F32),
            pltpu.VMEM((TP, 2, ROWS, 256), BF16), pltpu.VMEM((TP, 512, DM), BF16), pltpu.VMEM((PIECE, DM), F32),
            dma((10,)), dma((3, 2)), dma((3, 2)), dma((2, TP, 2)), dma((TP, 2, 4)), dma((TP, 2, 3)), dma((TP, 8, 2)), dma((2, TP, 4)), dma((TP, 4)),
        ],
        compiler_params=pltpu.CompilerParams(collective_id=0, has_side_effects=True, vmem_limit_bytes=58 * 1024 * 1024),
        name='layer',
    )(x, pos, gain, freq, wq, wk, wv, wo)


def finish_kernel(ya_ref, accb_ref, olast_ref, wlast_ref, kt_ref, vt_ref, y_out, kt_out, vt_out, yb, sem):
    copies = []

    def put(src, dst, i):
        copies.append(pltpu.make_async_copy(src, dst, sem.at[i]))
        copies[-1].start()

    put(ya_ref, y_out.at[pl.ds(0, PIECE)], 0)
    put(kt_ref, kt_out, 1)
    put(vt_ref, vt_out, 2)
    for t in range(4):
        cols = slice(t * 512, (t + 1) * 512)
        part = jnp.dot(olast_ref[...], wlast_ref[:, cols], preferred_element_type=F32)
        yb[:, cols] = (accb_ref[:, cols] + part).astype(BF16)
        put(yb.at[:, pl.ds(t * 512, 512)], y_out.at[pl.ds(PIECE, PIECE), pl.ds(t * 512, 512)], 3 + t)
    for cpy in copies:
        cpy.wait()


def finish(*parts):
    sds = jax.ShapeDtypeStruct
    return pl.pallas_call(
        finish_kernel,
        out_shape=(sds((ROWS, DM), BF16), sds((128, ROWS), BF16), sds((128, ROWS), BF16)),
        in_specs=[pl.BlockSpec(memory_space=pltpu.VMEM)] * 6,
        out_specs=(pl.BlockSpec(memory_space=pltpu.HBM),) * 3,
        scratch_shapes=[pltpu.VMEM((PIECE, DM), BF16), pltpu.SemaphoreType.DMA((7,))],
        compiler_params=pltpu.CompilerParams(vmem_limit_bytes=8 * 1024 * 1024),
        name='finish',
    )(*parts)


def solution(mesh):
    def local_step(x, doc_id, pos, gain, wq, wk, wv, wo, inv_freq):
        y, kt, vt = finish(*layer(x, pos.reshape(4, BLK), gain.reshape(1, DM), inv_freq.reshape(1, 32), wq, wk, wv, wo))
        return y, kt.T.reshape(ROWS, 2, 64), vt.T.reshape(ROWS, 2, 64)

    row_spec = P(('dp', 'cp'))
    in_specs = (P(('dp', 'cp'), None), row_spec, row_spec, P(), P(None, 'tp'), P(None, 'tp'), P(None, 'tp'), P('tp', None), P())
    out_specs = (P(('dp', 'cp'), None), P(('dp', 'cp'), 'tp', None), P(('dp', 'cp'), 'tp', None))
    return jax.shard_map(local_step, mesh=mesh, in_specs=in_specs, out_specs=out_specs, check_vma=False)
```
